32 devices in a mesh: slab: 8 (over y, x, core), tile: 4 (over z).
Axes of the slice: x: 2, y: 2, z: 4, core: 2. Of those that a mesh axis runs over, the one named last changes fastest.
Arguments:
- volume: float32 [128, 256, 1024], P('slab', 'tile'), may hold values from -0.3 to 0.3
- shears: float32 [8], replicated, may hold values from -0.4 to 0.4
- tile_shift: int32 [8, 4], P(None, 'tile'), may hold values from -1 to 1
- illumination: float32 [2, 128, 128], replicated, may hold values from -6 to 6
- measured: bfloat16 [1024, 128, 128], P(('slab', 'tile')), may hold values from 0.049804688 to 2.5
- frame_owner: int32 [1024, 1], P(('slab', 'tile')), may hold values from 0 to 7; in each aligned block of 32 rows (0 to 31, 32 to 63, ...) at most 8 rows name the same one
- frame_shift: int32 [1024], P(('slab', 'tile')), may hold values from -32 to 160
Outputs:
- volume_grad: float32 [128, 256, 1024], P('slab', 'tile')
The draws below stay inside these ranges and needn't reach their ends.
Inputs may be any that keep to these rules, and one draw needn't show every extreme that they name: `frame_owner`: the 32 frames of one device name each angle at most 8 times, a bound that some block reaches.
All inputs are finite; a program needn't handle non-finite values.
Results may differ from the reference program's by a relative error of at most 0.012.
Values may be sent and summed in bfloat16 or wider, within the bound.
A program may use at most 256 MiB of HBM per device.

```python
import math
import jax
import jax.numpy as jnp
import numpy as np
from jax import lax

SIDE = 128
SLICES = 128
GRID = 1024
BLOCK = 128
HALO = 32
ZT_DEV = 64
FR_DEV = 32
NZ = 256
ANGLES = 8
NFR = 1024
CAP = 8
N_SLAB = 8
N_TILE = 4


def set_ends(values, key, least, top_value):
    longest = values.shape.index(max(values.shape))
    spots = []
    for shift in (0, 1):
        where = [jax.random.randint(jax.random.fold_in(key, axis), (), 0, length) for axis, length in enumerate(values.shape)]
        where[longest] = (where[longest] + shift) % values.shape[longest]
        spots.append(tuple(where))
    return values.at[spots[0]].set(least).at[spots[1]].set(top_value)


def levels(key, extent, shards, smallest, high):
    def one(dim, blocks):
        draws = jax.random.uniform(jax.random.fold_in(jax.random.fold_in(key, 6), dim), (blocks,), jnp.float32, smallest / len(shards), high / len(shards))
        return jnp.repeat(jnp.exp(draws), extent[dim] // blocks).reshape((-1,) + (1,) * (len(extent) - dim - 1))

    gain = one(*shards[0])
    for cut in shards[1:]:
        gain = gain * one(*cut)
    return gain


def assign_block(stream_key, own, number, rows, count, top, reach, slope):
    order = jax.random.permutation(stream_key, count)
    heavy_load, usual = shares(count, rows * top, reach, slope, True), shares(count, rows * top, reach, slope, False)
    places = jnp.arange(count)

    def named(tallies, turn):
        used = int((tallies > 0).sum())
        fixed = max(1, used // 4)
        moved = fixed + (places - fixed + turn * (used - fixed)) % max(1, count - fixed)
        return jnp.zeros((count,), jnp.int32).at[order[jnp.where(places < fixed, places, moved)]].set(jnp.asarray(tallies, jnp.int32))

    tallies = jnp.where(number % 4 == 0, named(heavy_load, number // 4), named(usual, number - number // 4 - 1))
    mixed = jax.random.permutation(jax.random.fold_in(own, 3), count)
    source_of, taker = mixed[0:count // 2 * 2:2], mixed[1:count // 2 * 2:2]
    room = jnp.minimum(tallies[source_of] - 1, reach - tallies[taker]) // 2
    room = jnp.where((source_of == order[0]) | (taker == order[0]) | (tallies[taker] == 0), 0, jnp.maximum(room, 0))
    moved = jax.random.randint(jax.random.fold_in(own, 4), (count // 2,), 0, 1 << 20) % (room + 1)
    tallies = tallies.at[source_of].add(-moved).at[taker].add(moved)
    items = jnp.searchsorted(jnp.cumsum(tallies), jnp.arange(rows * top), side="right").astype(jnp.int32)
    grid = items.reshape(top, rows).T
    grid = grid[jax.random.permutation(jax.random.fold_in(own, 1), rows)]
    turn = jax.random.randint(jax.random.fold_in(own, 2), (rows, 1), 0, top)
    return jnp.take_along_axis(grid, (jnp.arange(top)[None, :] + turn) % top, axis=1)


def shares(amount, total, bound, lean, full):
    portions = [(1 << 20) // math.isqrt(rank ** lean) + 1 for rank in range(1, amount + 1)]
    largest = bound if full else min(bound, max(-(-total // amount), total * portions[0] // sum(portions)))
    least = 1 if total - largest >= amount - 1 else 0
    holding, rest = [largest] + [least] * (amount - 1), total - largest - least * (amount - 1)
    while rest > 0:
        free = [i for i in range(1, amount) if holding[i] < largest] or [i for i in range(1, amount) if holding[i] < bound]
        pool, left = sum([portions[i] for i in free]), rest
        for i in free:
            more = min(bound - holding[i], max(1, left * portions[i] // pool), rest)
            holding[i] = holding[i] + more
            rest = rest - more
    return np.array(holding)


def bell_draw(stream_key, extent, width, bound, split=(), kind=jnp.bfloat16):
    entries = jax.random.normal(stream_key, extent, jnp.float32) * width
    if len(split) > 0:
        entries = levels(stream_key, extent, split, -0.22, 0.18) * entries
    return jnp.clip(entries, min=-bound, max=bound).astype(kind)


def setup_inputs(seed: int = 0) -> dict:
    splits = jax.random.split(jax.random.key(seed), 8)
    volume = bell_draw(splits[0], (SLICES, NZ, GRID), 0.05, 0.3, ((0, 8), (1, 4)), jnp.float32)
    shears = jnp.clip(jax.random.uniform(splits[1], (ANGLES,), jnp.float32, -0.4, 0.4), -0.4, 0.4)
    tile_shift = set_ends(jax.random.randint(splits[2], (ANGLES, N_TILE), -1, 2), jax.random.fold_in(splits[2], 1), -1, 1).astype(jnp.int32)
    illumination = bell_draw(splits[3], (2, SIDE, SIDE), 1.0, 6.0, (), jnp.float32)
    measured = jnp.clip(0.049804688 + 2.4501953 * jax.random.uniform(splits[4], (NFR, SIDE, SIDE), jnp.float32) ** levels(splits[4], (NFR, SIDE, SIDE), ((0, 32),), -0.2, 0.2), 0.049804688, 2.5).astype(jnp.bfloat16)
    frame_owner_keys = jax.random.split(jax.random.fold_in(splits[5], 1), NFR // FR_DEV)
    frame_owner_turns = jax.random.permutation(jax.random.fold_in(splits[5], 3), NFR // FR_DEV)
    frame_owner = jax.vmap(lambda own, number: assign_block(jax.random.fold_in(splits[5], 2), own, number, FR_DEV, N_SLAB, 1, CAP, 2))(frame_owner_keys, frame_owner_turns).reshape((NFR, 1))
    frame_shift = set_ends(jax.random.randint(splits[6], (NFR,), -HALO, GRID // N_TILE - SIDE + HALO + 1), jax.random.fold_in(splits[6], 1), -HALO, (GRID // N_TILE - SIDE + HALO + 1) - 1).astype(jnp.int32)
    return dict(volume=volume, shears=shears, tile_shift=tile_shift, illumination=illumination, measured=measured, frame_owner=frame_owner, frame_shift=frame_shift)


smoothing = 0.25
highest = lax.Precision.HIGHEST

def beam_kernel(shear_one, beam_depth, block_width):
    beam_pos = jnp.arange(beam_depth, dtype=jnp.float32)
    centre = block_width * 0.5 + (beam_pos - (beam_depth - 1) * 0.5) * shear_one
    source = jnp.arange(block_width, dtype=jnp.float32)
    target = jnp.arange(2 * block_width, dtype=jnp.float32)
    spread = target[None, None, :] - source[None, :, None] - centre[:, None, None]
    values = jnp.exp(-0.5 * spread * spread).astype(jnp.bfloat16)
    return values.reshape(beam_depth * block_width, 2 * block_width)

def dft_tables(length):
    indices = jnp.arange(length, dtype=jnp.int32)
    product = indices[:, None] * indices[None, :] % length
    phases = product.astype(jnp.float32) * (2.0 * math.pi / length)
    return (jnp.cos(phases), jnp.sin(phases))

def left_mul(matrix, frames_in):
    return jnp.einsum('jk,nkl->njl', matrix, frames_in, precision=highest)

def right_mul(frames_in, matrix):
    return jnp.einsum('njk,kl->njl', frames_in, matrix, precision=highest)

def phase_gradient(windows, illumination, amplitude, dft_cos, dft_sin):
    length = dft_cos.shape[0]
    object_re = jnp.cos(windows)
    object_im = jnp.sin(windows)
    probe_re = illumination[0]
    probe_im = illumination[1]
    wave_re = probe_re * object_re - probe_im * object_im
    wave_im = probe_re * object_im + probe_im * object_re
    half_re = left_mul(dft_cos, wave_re) + left_mul(dft_sin, wave_im)
    half_im = left_mul(dft_cos, wave_im) - left_mul(dft_sin, wave_re)
    far_re = (right_mul(half_re, dft_cos) + right_mul(half_im, dft_sin)) / length
    far_im = (right_mul(half_im, dft_cos) - right_mul(half_re, dft_sin)) / length
    modulus = jnp.sqrt(far_re * far_re + far_im * far_im + smoothing)
    factor = 1.0 - amplitude / modulus
    resid_re = far_re * factor
    resid_im = far_im * factor
    back_re = left_mul(dft_cos, resid_re) - left_mul(dft_sin, resid_im)
    back_im = left_mul(dft_cos, resid_im) + left_mul(dft_sin, resid_re)
    near_re = (right_mul(back_re, dft_cos) - right_mul(back_im, dft_sin)) / length
    near_im = (right_mul(back_im, dft_cos) + right_mul(back_re, dft_sin)) / length
    grad_re = probe_re * near_re + probe_im * near_im
    grad_im = probe_re * near_im - probe_im * near_re
    return grad_im * object_re - grad_re * object_im

def reference(volume, shears, tile_shift, illumination, measured, frame_owner, frame_shift):
    blocks_row = GRID // BLOCK
    own_width = GRID // N_TILE
    block_ids = jnp.arange(blocks_row, dtype=jnp.int32)
    volume_half = lax.optimization_barrier(volume.astype(jnp.bfloat16))

    def make_kernel(shear_one):
        return beam_kernel(shear_one, ZT_DEV, BLOCK)
    kernels = lax.optimization_barrier(lax.map(make_kernel, shears))

    def selector(offset, plus_one):
        return (block_ids[:, None] == block_ids[None, :] + offset + plus_one).astype(jnp.float32)

    def project_angle(angle_id):
        kernel_wide = kernels[angle_id].astype(jnp.float32)

        def per_tile(running, tile_id):
            part_volume = lax.dynamic_slice_in_dim(volume_half, tile_id * ZT_DEV, ZT_DEV, 1)
            rows_matrix = part_volume.reshape(SLICES, ZT_DEV, blocks_row, BLOCK).transpose(0, 2, 1, 3)
            rows_matrix = rows_matrix.reshape(SLICES * blocks_row, ZT_DEV * BLOCK).astype(jnp.float32)
            partial_sum = jnp.dot(rows_matrix, kernel_wide, precision=highest).reshape(SLICES, blocks_row, 2, BLOCK)
            offset = tile_shift[angle_id, tile_id]
            shifted = jnp.einsum('ki,sib->skb', selector(offset, 0), partial_sum[:, :, 0], precision=highest)
            shifted = shifted + jnp.einsum('ki,sib->skb', selector(offset, 1), partial_sum[:, :, 1], precision=highest)
            return (running + shifted, None)
        initial = jnp.zeros((SLICES, blocks_row, BLOCK), jnp.float32)
        running, unused = lax.scan(per_tile, initial, jnp.arange(N_TILE, dtype=jnp.int32))
        return running.reshape(SLICES, GRID)
    projection = lax.map(project_angle, jnp.arange(ANGLES, dtype=jnp.int32))
    phase_pad = jnp.pad(projection, ((0, 0), (0, 0), (HALO, HALO)))
    dft_cos, dft_sin = dft_tables(SIDE)
    frame_ids = jnp.arange(NFR, dtype=jnp.int32)
    starts = frame_ids // FR_DEV % N_TILE * own_width + frame_shift + HALO
    angles = frame_owner[:, 0]
    batches = NFR // FR_DEV
    zero_index = jnp.zeros((), jnp.int32)

    def one_batch(grad_pad, batch_data):
        angle_batch, start_batch, amp_batch = batch_data

        def cut_one(angle_id, start_col):
            return lax.dynamic_slice(phase_pad[angle_id], (zero_index, start_col), (SIDE, SIDE))
        windows = jax.vmap(cut_one)(angle_batch, start_batch)
        dphase = phase_gradient(windows, illumination, amp_batch.astype(jnp.float32), dft_cos, dft_sin)

        def add_one(member, current):
            corner = (angle_batch[member], zero_index, start_batch[member])
            current_piece = lax.dynamic_slice(current, corner, (1, SIDE, SIDE))
            return lax.dynamic_update_slice(current, current_piece + dphase[member][None], corner)
        return (lax.fori_loop(0, FR_DEV, add_one, grad_pad), None)
    grad_initial = jnp.zeros_like(phase_pad)
    batch_inputs = (angles.reshape(batches, FR_DEV), starts.reshape(batches, FR_DEV), measured.reshape(batches, FR_DEV, SIDE, SIDE))
    grad_pad, unused = lax.scan(one_batch, grad_initial, batch_inputs)
    proj_grad = lax.optimization_barrier(grad_pad[:, :, HALO:HALO + GRID].astype(jnp.bfloat16))
    proj_wide = proj_grad.astype(jnp.float32).reshape(ANGLES, SLICES, blocks_row, BLOCK)

    def back_tile(tile_id):

        def per_angle(running, angle_id):
            kernel_wide = kernels[angle_id].astype(jnp.float32)
            offset = tile_shift[angle_id, tile_id]
            grad_rows = proj_wide[angle_id]
            pick_low = jnp.einsum('ki,skb->sib', selector(offset, 0), grad_rows, precision=highest)
            pick_high = jnp.einsum('ki,skb->sib', selector(offset, 1), grad_rows, precision=highest)
            stacked = jnp.concatenate([pick_low, pick_high], axis=2).reshape(SLICES * blocks_row, 2 * BLOCK)
            return (running + jnp.dot(stacked, kernel_wide.T, precision=highest), None)
        initial = jnp.zeros((SLICES * blocks_row, ZT_DEV * BLOCK), jnp.float32)
        running, unused = lax.scan(per_angle, initial, jnp.arange(ANGLES, dtype=jnp.int32))
        return running.reshape(SLICES, blocks_row, ZT_DEV, BLOCK).transpose(0, 2, 1, 3).reshape(SLICES, ZT_DEV, GRID)
    tile_grads = lax.map(back_tile, jnp.arange(N_TILE, dtype=jnp.int32))
    return tile_grads.transpose(1, 0, 2, 3).reshape(SLICES, NZ, GRID)
```

```python
import math

import jax
import jax.numpy as jnp
from jax import lax
from jax.experimental import pallas as pl
from jax.experimental.pallas import tpu as pltpu
from jax.sharding import PartitionSpec as P

SIDE = 128
BLOCK = 128
HALO = 32
GRAD_T = jnp.bfloat16


smoothing = 0.25
precise = lax.Precision.HIGH


def extended(value, sides, width):
    for axis, dim in sides:
        count, length = (lax.axis_size(axis), value.shape[dim])
        up = [(i, (i + 1) % count) for i in range(count - 1)]
        down = [(j, i) for i, j in up]
        last = lax.slice_in_dim(value, length - width, length, axis=dim)
        first = lax.slice_in_dim(value, 0, width, axis=dim)
        before = lax.ppermute(last, axis, up)
        after = lax.ppermute(first, axis, down)
        value = jnp.concatenate([before, value, after], axis=dim)
    return value


def passed_along(value, axis, steps):
    count = lax.axis_size(axis)
    first, last = (max(0, -steps), min(count, count - steps))
    return lax.ppermute(value, axis, [(source, source + steps) for source in range(first, last)])


def beam_kernel(shear_one, beam_depth, block_width):
    beam_pos = jnp.arange(beam_depth, dtype=jnp.float32)
    centre = block_width * 0.5 + (beam_pos - (beam_depth - 1) * 0.5) * shear_one
    source = jnp.arange(block_width, dtype=jnp.float32)
    target = jnp.arange(2 * block_width, dtype=jnp.float32)
    spread = target[None, None, :] - source[None, :, None] - centre[:, None, None]
    values = jnp.exp(-0.5 * spread * spread).astype(jnp.bfloat16)
    return values.reshape(beam_depth * block_width, 2 * block_width)


def dft_tables(length):
    indices = jnp.arange(length, dtype=jnp.int32)
    product = indices[:, None] * indices[None, :] % length
    phases = product.astype(jnp.float32) * (2.0 * math.pi / length)
    return (jnp.cos(phases), jnp.sin(phases))


def left_mul(matrix, frames_in):
    return jnp.einsum("jk,nkl->njl", matrix, frames_in, precision=precise)


def right_mul(frames_in, matrix):
    return jnp.einsum("njk,kl->njl", frames_in, matrix, precision=precise)


def phase_gradient(windows, illumination, amplitude, dft_cos, dft_sin):
    length = dft_cos.shape[0]
    object_re = jnp.cos(windows)
    object_im = jnp.sin(windows)
    probe_re = illumination[0]
    probe_im = illumination[1]
    wave_re = probe_re * object_re - probe_im * object_im
    wave_im = probe_re * object_im + probe_im * object_re
    half_re = left_mul(dft_cos, wave_re) + left_mul(dft_sin, wave_im)
    half_im = left_mul(dft_cos, wave_im) - left_mul(dft_sin, wave_re)
    far_re = (right_mul(half_re, dft_cos) + right_mul(half_im, dft_sin)) / length
    far_im = (right_mul(half_im, dft_cos) - right_mul(half_re, dft_sin)) / length
    modulus = jnp.sqrt(far_re * far_re + far_im * far_im + smoothing)
    factor = 1.0 - amplitude / modulus
    resid_re = far_re * factor
    resid_im = far_im * factor
    back_re = left_mul(dft_cos, resid_re) - left_mul(dft_sin, resid_im)
    back_im = left_mul(dft_cos, resid_im) + left_mul(dft_sin, resid_re)
    near_re = (right_mul(back_re, dft_cos) - right_mul(back_im, dft_sin)) / length
    near_im = (right_mul(back_im, dft_cos) + right_mul(back_re, dft_sin)) / length
    grad_re = probe_re * near_re + probe_im * near_im
    grad_im = probe_re * near_im - probe_im * near_re
    return grad_im * object_re - grad_re * object_im


def moved_blocks(value, offsets, axis, start, count):
    ahead = jnp.reshape(offsets, offsets.shape + (1,) * (value.ndim - 1))
    cuts = [lax.slice_in_dim(value, start + step, start + step + count, axis=axis) for step in (-1, 0, 1)]
    return jnp.where(ahead < 0, cuts[0], jnp.where(ahead > 0, cuts[2], cuts[1]))


def frame_adder(owner_ref, start_ref, grads_ref, out_ref):
    frames, rows, width = grads_ref.shape
    out_ref[...] = jnp.zeros_like(out_ref)
    lanes = lax.broadcasted_iota(jnp.int32, (rows, width), 1)

    def add_one(member, carried):
        angle = owner_ref[member]
        first = start_ref[member]
        block = first // width
        shift = first - block * width
        turned = pltpu.roll(grads_ref[member], shift, 1)
        kept = lanes >= shift
        out_ref[angle, block] += jnp.where(kept, turned, 0.0)
        out_ref[angle, block + 1] += jnp.where(kept, 0.0, turned)
        return carried

    lax.fori_loop(0, frames, add_one, 0)


def add_frames(owners, starts, grads, angles, pad_width):
    frames, rows, width = grads.shape
    blocks = pad_width // width + 1
    summed = pl.pallas_call(
        frame_adder,
        out_shape=jax.ShapeDtypeStruct((angles, blocks, rows, width), jnp.float32),
        in_specs=[
            pl.BlockSpec(memory_space=pltpu.SMEM),
            pl.BlockSpec(memory_space=pltpu.SMEM),
            pl.BlockSpec(memory_space=pltpu.VMEM),
        ],
        out_specs=pl.BlockSpec(memory_space=pltpu.VMEM),
        compiler_params=pltpu.CompilerParams(vmem_limit_bytes=32 * 1024 * 1024),
        name="add_frames",
    )(owners, starts, grads)
    summed = summed.transpose(0, 2, 1, 3).reshape(angles, rows, blocks * width)
    return summed[:, :, :pad_width]


def body(volume, shears, tile_shift, illumination, measured, frame_owner, frame_shift):
    slices_dev, beam_depth, grid_width = volume.shape
    blocks_row = grid_width // BLOCK
    volume_rows = volume.astype(jnp.bfloat16).reshape(slices_dev, beam_depth, blocks_row, BLOCK)
    volume_rows = volume_rows.transpose(0, 2, 1, 3).reshape(
        slices_dev * blocks_row, beam_depth * BLOCK
    )
    offsets = tile_shift[:, 0]

    def project_angle(carried, shear_one):
        kernel = beam_kernel(shear_one, beam_depth, BLOCK)
        partial_sum = jnp.dot(volume_rows, kernel, preferred_element_type=jnp.float32)
        return (carried, (partial_sum, kernel))

    unused, (sums, kernels) = lax.scan(project_angle, jnp.zeros((), jnp.float32), shears)
    angles = sums.shape[0]
    sums = sums.reshape(angles, slices_dev, blocks_row, 2, BLOCK)
    low = jnp.pad(sums[:, :, :, 0], ((0, 0), (0, 0), (1, 2), (0, 0)))
    high = jnp.pad(sums[:, :, :, 1], ((0, 0), (0, 0), (2, 1), (0, 0)))
    partials = moved_blocks(low + high, -offsets, 2, 1, blocks_row)
    partials = partials.reshape(angles, slices_dev, grid_width)
    landed = lax.psum_scatter(partials, "tile", scatter_dimension=2, tiled=True)
    landed = lax.all_to_all(landed, "slab", split_axis=0, concat_axis=1, tiled=True)
    phase_own = landed[0]
    phase_pad = extended(phase_own, (("tile", 1),), HALO)
    row_count, pad_width = phase_pad.shape
    own_width = pad_width - 2 * HALO
    dft_cos, dft_sin = dft_tables(SIDE)
    zero_index = jnp.zeros((), jnp.int32)
    frames_dev = measured.shape[0]
    owners = frame_owner[:, 0]
    every_phase = lax.all_gather(phase_pad[None], "slab", axis=0, tiled=True)
    frame_starts = frame_shift + HALO

    def cut_frame(angle_id, start_col):
        return lax.dynamic_slice(
            every_phase, (angle_id, zero_index, start_col), (1, row_count, SIDE)
        )[0]

    windows = jax.vmap(cut_frame)(owners, frame_starts)
    dphase = phase_gradient(windows, illumination, measured.astype(jnp.float32), dft_cos, dft_sin)

    per_angle = add_frames(owners, frame_starts, dphase, every_phase.shape[0], pad_width)
    grad_pad = lax.psum_scatter(per_angle.astype(GRAD_T), "slab", scatter_dimension=0, tiled=True)[0]
    grad_pad = grad_pad.astype(jnp.float32)
    from_left = passed_along(grad_pad[:, HALO + own_width :], "tile", 1)
    from_right = passed_along(grad_pad[:, :HALO], "tile", -1)
    own_part = grad_pad[:, HALO : HALO + own_width]
    own_part = own_part.at[:, :HALO].add(from_left)
    own_part = own_part.at[:, own_width - HALO :].add(from_right)
    proj_grad = own_part.astype(jnp.bfloat16)[None]
    spread = lax.all_to_all(proj_grad, "slab", split_axis=1, concat_axis=0, tiled=True)
    spread = lax.all_gather(spread, "tile", axis=2, tiled=True)

    pieces = spread.reshape(angles, slices_dev, blocks_row, BLOCK)
    pieces = jnp.pad(pieces, ((0, 0), (0, 0), (1, 2), (0, 0)))
    stacks = jnp.concatenate(
        [
            moved_blocks(pieces, offsets, 2, 1, blocks_row),
            moved_blocks(pieces, offsets, 2, 2, blocks_row),
        ],
        axis=3,
    ).reshape(angles, slices_dev * blocks_row, 2 * BLOCK)

    def back_angle(running, inputs):
        kernel, stacked = inputs
        update = lax.dot_general(
            stacked, kernel, (((1,), (1,)), ((), ())), preferred_element_type=jnp.float32
        )
        return (running + update, None)

    initial = jnp.zeros((slices_dev * blocks_row, beam_depth * BLOCK), jnp.float32)
    running, unused = lax.scan(back_angle, initial, (kernels, stacks))
    running = running.reshape(slices_dev, blocks_row, beam_depth, BLOCK).transpose(0, 2, 1, 3)
    return running.reshape(slices_dev, beam_depth, grid_width)


def solution(mesh):
    in_specs = (
        P("slab", "tile", None),
        P(),
        P(None, "tile"),
        P(),
        P(("slab", "tile"), None, None),
        P(("slab", "tile"), None),
        P(("slab", "tile")),
    )
    out_specs = P("slab", "tile", None)
    return jax.shard_map(body, mesh=mesh, in_specs=in_specs, out_specs=out_specs, check_vma=False)
```
